8 devices in a mesh: model: 2 (over z, y), data: 4 (over x, core).
Axes of the slice: x: 2, y: 2, z: 1, core: 2. Of those that a mesh axis runs over, the one named last changes fastest.
Arguments:
- x_in: bfloat16 [64, 128, 2048], P('data')
- cot_out: bfloat16 [64, 128, 2048], P('data')
- step_emb: bfloat16 [2, 2048], replicated
- w_q: bfloat16 [2048, 2048], P(None, 'model')
- w_k: bfloat16 [2048, 2048], P(None, 'model')
- w_v: bfloat16 [2048, 2048], P(None, 'model')
- w_o: bfloat16 [2048, 2048], P('model')
- w_1: bfloat16 [2048, 8192], P(None, 'model')
- w_2: bfloat16 [8192, 2048], P('model')
Outputs:
- output 1: float32 [2048, 2048], P(None, 'model')
- output 2: float32 [2048, 2048], P(None, 'model')
- output 3: float32 [2048, 2048], P(None, 'model')
- output 4: float32 [2048, 2048], P('model')
- output 5: float32 [2048, 8192], P(None, 'model')
- output 6: float32 [8192, 2048], P('model')
- output 7: bfloat16 [64, 128, 2048], P('data')
All inputs are finite; a program needn't handle non-finite values.
Results may differ from the reference program's by a relative error of at most 0.0184834.
Values are sent between devices in bfloat16 or wider.
A program may use at most 1 GiB of HBM per device.

```python
import jax
import jax.numpy as jnp
from jax import lax

BATCH = 64
SEQ = 128
D = 2048
HEADS = 32
FF = 8192
LAYERS = 2


def normal_weight(key, rows, cols):
    return (jax.random.normal(key, (rows, cols), jnp.float32) * rows ** -0.5).astype(jnp.bfloat16)


def setup_inputs(seed: int = 0) -> dict:
    key_list = jax.random.split(jax.random.key(seed), 9)
    x_in = jax.random.normal(key_list[0], (BATCH, SEQ, D), jnp.float32).astype(jnp.bfloat16)
    cot_out = jax.random.normal(key_list[1], (BATCH, SEQ, D), jnp.float32).astype(jnp.bfloat16)
    step_emb = (0.5 * jax.random.normal(key_list[2], (LAYERS, D), jnp.float32)).astype(jnp.bfloat16)
    return dict(x_in=x_in, cot_out=cot_out, step_emb=step_emb,
                w_q=normal_weight(key_list[3], D, D), w_k=normal_weight(key_list[4], D, D),
                w_v=normal_weight(key_list[5], D, D), w_o=normal_weight(key_list[6], D, D),
                w_1=normal_weight(key_list[7], D, FF), w_2=normal_weight(key_list[8], FF, D))


def rms_norm(values):
    return values * lax.rsqrt(jnp.mean(values * values, axis=-1, keepdims=True) + 1e-6)


def attend_one(qkv_seq):
    q_seq, k_seq, v_seq = qkv_seq
    head_dim = q_seq.shape[-1]
    scores = jnp.einsum('qhe,khe->hqk', q_seq, k_seq) * (head_dim ** -0.5)
    prob_mat = jax.nn.softmax(scores, axis=-1).astype(jnp.bfloat16).astype(jnp.float32)
    return jnp.einsum('hqk,khe->qhe', prob_mat, v_seq).astype(jnp.bfloat16)


def shared_block(x_cur, step_vec, weights32):
    w_q, w_k, w_v, w_o, w_1, w_2 = weights32
    batch_size, seq_len, width_model = x_cur.shape
    head_shape = (batch_size, seq_len, HEADS, width_model // HEADS)
    x_f = x_cur.astype(jnp.float32) + step_vec.astype(jnp.float32)
    u_f = rms_norm(x_f).astype(jnp.bfloat16).astype(jnp.float32)
    q_all = jnp.einsum('bsd,de->bse', u_f, w_q).astype(jnp.bfloat16).astype(jnp.float32).reshape(head_shape)
    k_all = jnp.einsum('bsd,de->bse', u_f, w_k).astype(jnp.bfloat16).astype(jnp.float32).reshape(head_shape)
    v_all = jnp.einsum('bsd,de->bse', u_f, w_v).astype(jnp.bfloat16).astype(jnp.float32).reshape(head_shape)
    context = lax.map(jax.checkpoint(attend_one), (q_all, k_all, v_all))
    context_f = context.reshape(batch_size, seq_len, width_model).astype(jnp.float32)
    h_f = (x_f + jnp.einsum('bse,ed->bsd', context_f, w_o)).astype(jnp.bfloat16).astype(jnp.float32)
    m_f = rms_norm(h_f).astype(jnp.bfloat16).astype(jnp.float32)
    z_b = jnp.einsum('bsd,df->bsf', m_f, w_1).astype(jnp.bfloat16)
    g_f = jax.nn.gelu(z_b.astype(jnp.float32)).astype(jnp.bfloat16).astype(jnp.float32)
    return (h_f + jnp.einsum('bsf,fd->bsd', g_f, w_2)).astype(jnp.bfloat16)


def reference(x_in, cot_out, step_emb, w_q, w_k, w_v, w_o, w_1, w_2):
    weights32 = tuple(weight.astype(jnp.float32) for weight in (w_q, w_k, w_v, w_o, w_1, w_2))

    def forward(x_start, weight_set):
        def scan_body(x_cur, step_vec):
            return jax.checkpoint(shared_block)(x_cur, step_vec, weight_set), None
        x_last, _ = lax.scan(scan_body, x_start, step_emb)
        return x_last

    _, pull_back = jax.vjp(forward, x_in, weights32)
    d_x, d_w = pull_back(cot_out)
    return (d_w[0], d_w[1], d_w[2], d_w[3], d_w[4], d_w[5], d_x)
```

```python
import jax
import jax.numpy as jnp
from jax import lax
from jax.sharding import PartitionSpec as P

HEAD_DIM = 64
EPS_NORM = 1e-6
CHUNK = 1024
F32 = jnp.float32
BF16 = jnp.bfloat16


SWAP_MODEL = ((0, 1), (1, 0))
SWAP_CORE = ((0, 1), (1, 0), (2, 3), (3, 2))
SWAP_CHIP = ((0, 2), (2, 0), (1, 3), (3, 1))


def swap_model(values):
    return lax.ppermute(values, 'model', SWAP_MODEL)


def swap_core(values):
    return lax.ppermute(values, 'data', SWAP_CORE)


def swap_chip(values):
    return lax.ppermute(values, 'data', SWAP_CHIP)


def ordered(index, mine, other, axis):
    return jnp.where(index == 0, jnp.concatenate([mine, other], axis), jnp.concatenate([other, mine], axis))


def rms_norm(values):
    return values * lax.rsqrt(jnp.mean(values * values, axis=-1, keepdims=True) + EPS_NORM)


def dot(lhs, rhs, lhs_dim, rhs_dim):
    return lax.dot_general(lhs, rhs, (((lhs_dim,), (rhs_dim,)), ((), ())), preferred_element_type=F32)


def split_heads(qkv, batch, seq):
    stacked = qkv.reshape(batch, seq, 3, qkv.shape[1] // (3 * HEAD_DIM), HEAD_DIM)
    return stacked[:, :, 0], stacked[:, :, 1], stacked[:, :, 2]


def attn_probs(q_head, k_head):
    scores = jnp.einsum('bqhe,bkhe->bhqk', q_head, k_head, preferred_element_type=F32)
    return jax.nn.softmax(scores * (HEAD_DIM ** -0.5), axis=-1)


def attn_forward(qkv, batch, seq):
    q_head, k_head, v_head = split_heads(qkv, batch, seq)
    prob_mat = attn_probs(q_head, k_head).astype(BF16)
    context = jnp.einsum('bhqk,bkhe->bqhe', prob_mat, v_head, preferred_element_type=F32)
    return context.astype(BF16).reshape(batch * seq, -1)


def attn_backward(qkv, d_context, batch, seq):
    q_head, k_head, v_head = split_heads(qkv, batch, seq)
    d_context = d_context.reshape(q_head.shape)
    prob_f = attn_probs(q_head, k_head)
    d_prob = jnp.einsum('bqhe,bkhe->bhqk', d_context, v_head, preferred_element_type=F32).astype(BF16).astype(F32)
    d_value = jnp.einsum('bhqk,bqhe->bkhe', prob_f.astype(BF16), d_context, preferred_element_type=F32).astype(BF16)
    d_scores = (prob_f * (d_prob - jnp.sum(prob_f * d_prob, axis=-1, keepdims=True)) * (HEAD_DIM ** -0.5)).astype(BF16)
    d_query = jnp.einsum('bhqk,bkhe->bqhe', d_scores, k_head, preferred_element_type=F32).astype(BF16)
    d_key = jnp.einsum('bhqk,bqhe->bkhe', d_scores, q_head, preferred_element_type=F32).astype(BF16)
    return tuple(part.reshape(batch * seq, -1) for part in (d_query, d_key, d_value))


def layer_forward(x_cur, step_vec, weights, batch, seq, last):
    w_qkv, w_out, w_up, w_down = weights
    x_f = x_cur.astype(F32) + step_vec.astype(F32)
    u_in = rms_norm(x_f).astype(BF16)
    qkv = [dot(u_in, w, 1, 0).astype(BF16) for w in w_qkv]
    context = [attn_forward(part, batch, seq) for part in qkv]
    attn_out = sum(dot(c, w, 1, 0) for c, w in zip(context, w_out))
    h_mid = (x_f + attn_out).astype(BF16)
    m_in = rms_norm(h_mid.astype(F32)).astype(BF16)
    z_up = [dot(m_in, w, 1, 0).astype(BF16) for w in w_up]
    g_act = [jax.nn.gelu(z.astype(F32)).astype(BF16) for z in z_up]
    x_next = None
    if not last:
        x_next = (h_mid.astype(F32) + sum(dot(g, w, 1, 0) for g, w in zip(g_act, w_down))).astype(BF16)
    return x_next, (x_cur, u_in, qkv, context, h_mid, m_in, z_up, g_act)


def layer_backward(d_next, step_vec, saved_acts, weights, batch, seq, step):
    w_qkv, w_out, w_up, w_down = weights
    x_cur, u_in, qkv, context, h_mid, m_in, z_up, g_act = saved_acts
    d_next = step('down', d_next, (g_act, d_next))
    d_up = []
    for z, w in zip(z_up, w_down):
        d_act = dot(d_next, w, 1, 1).astype(BF16)
        d_up.append(jax.vjp(jax.nn.gelu, z.astype(F32))[1](d_act.astype(F32))[0].astype(BF16))
    d_up = step('up', d_up, (d_up, m_in))
    d_norm2 = sum(dot(d, w, 1, 1) for d, w in zip(d_up, w_up)).astype(BF16)
    norm_pull = jax.vjp(rms_norm, h_mid.astype(F32))[1]
    d_mid = (d_next.astype(F32) + norm_pull(d_norm2.astype(F32))[0]).astype(BF16)
    d_mid = step('out', d_mid, (context, d_mid))
    d_context = [dot(d_mid, w, 1, 1).astype(BF16) for w in w_out]
    d_heads = [attn_backward(part, d, batch, seq) for part, d in zip(qkv, d_context)]
    d_heads = step('qkv', d_heads, (d_heads, u_in))
    d_qkv = [jnp.concatenate(d, axis=1) for d in d_heads]
    d_norm1 = sum(dot(d, w, 1, 1) for d, w in zip(d_qkv, w_qkv)).astype(BF16)
    x_f = x_cur.astype(F32) + step_vec.astype(F32)
    norm_pull_x = jax.vjp(rms_norm, x_f)[1]
    return (d_mid.astype(F32) + norm_pull_x(d_norm1.astype(F32))[0]).astype(BF16)


class GradientPipe:
    def __init__(self, core_idx, chip_idx):
        self.core_idx, self.chip_idx = core_idx, chip_idx
        self.blocks, self.sent, self.done = [], [], 0

    def begin(self, name, p_first, p_layers, q_layers):
        q_all = jnp.concatenate(q_layers, axis=0)
        half_q = q_all.shape[1] // 2
        q_mine = lax.dynamic_slice_in_dim(q_all, self.core_idx * half_q, half_q, 1)
        q_mate = lax.dynamic_slice_in_dim(q_all, (1 - self.core_idx) * half_q, half_q, 1)

        def product(p_part, q_part):
            return dot(p_part, q_part, 0, 0) if p_first else dot(q_part, p_part, 0, 0)

        own_p = [jnp.concatenate(c, axis=0) for c in zip(*(columns(parts[:1]) for parts in p_layers))]
        other_p = [jnp.concatenate(c, axis=0) for c in zip(*(columns(parts[1:]) for parts in p_layers))]
        for own, other in zip(own_p, other_p):
            if len(self.sent) > 1:
                own, other, _ = lax.optimization_barrier((own, other, self.sent[-2]))
            send = product(other, q_mine) + swap_core(product(other, q_mate))
            from_core = swap_core(product(own, q_mate))
            self.sent.append(send)
            self.blocks.append(dict(name=name, axis=1 if p_first else 0, wait='model', arrives=swap_model(send),
                                    here=product(own, q_mine) + from_core))

    def after_sends(self, value):
        return lax.optimization_barrier((value, self.sent[-1]))[0]

    def stage(self, value=None):
        moving = [b for b in self.blocks[:self.done + 1] if b['wait']]
        self.done += 1
        got, value = lax.optimization_barrier(([b['arrives'] for b in moving], value))
        for block, arrived in zip(moving, got):
            axis = block['axis']
            if block['wait'] == 'model':
                total = block['here'] + arrived
                part = total.shape[axis] // 2
                block['here'] = lax.dynamic_slice_in_dim(total, self.chip_idx * part, part, axis)
                give = lax.dynamic_slice_in_dim(total, (1 - self.chip_idx) * part, part, axis)
                block.update(wait='chip', arrives=swap_chip(give))
            elif block['wait'] == 'chip':
                block['here'] = block['here'] + arrived
                block.update(wait='share', arrives=swap_chip(block['here']))
            elif block['wait'] == 'share':
                block['here'] = ordered(self.chip_idx, block['here'], arrived, axis)
                block.update(wait='core', arrives=swap_core(block['here']))
            else:
                block['here'] = ordered(self.core_idx, block['here'], arrived, axis)
                block['wait'] = None
        return value

    def finish(self):
        while any(b['wait'] for b in self.blocks):
            self.stage()

    def result(self, name):
        mine = [b for b in self.blocks if b['name'] == name]
        return mine[0]['here'] if len(mine) == 1 else jnp.concatenate([b['here'] for b in mine], axis=1 - mine[0]['axis'])


def columns(parts):
    return [p[:, start:start + CHUNK] for p in parts for start in range(0, p.shape[1], CHUNK)]


def solution(mesh):
    spec_col = P(None, 'model')
    spec_row = P('model', None)
    spec_act = P('data', None, None)
    spec_rep = P(None, None)

    def device_step(x_in, cot_out, step_emb, w_q, w_k, w_v, w_o, w_1, w_2):
        model_idx = lax.axis_index('model')
        data_idx = lax.axis_index('data')
        chip_idx = data_idx // 2
        core_idx = data_idx % 2
        batch, seq, width = x_in.shape[0] // 2, x_in.shape[1], x_in.shape[2]
        layer_count = step_emb.shape[0]

        def from_neighbour(*shards):
            rows = shards[0].shape[0] // 4
            start = (core_idx * 2 + chip_idx) * rows
            return swap_model(jnp.concatenate([lax.dynamic_slice_in_dim(s, start, rows, 0) for s in shards], axis=1))

        def shared(got):
            pair = ordered(chip_idx, got, swap_chip(got), 0)
            return ordered(core_idx, pair, swap_core(pair), 0)

        half = w_2.shape[0] // 2
        got_qkv = from_neighbour(w_q, w_k, w_v)
        got_out = from_neighbour(w_o)
        got_up = [from_neighbour(w_1[:, i * half:(i + 1) * half]) for i in (0, 1)]
        got_down = [from_neighbour(w_2[i * half:(i + 1) * half]) for i in (0, 1)]
        weights = ((jnp.concatenate([w_q, w_k, w_v], axis=1), shared(got_qkv)), (w_o, shared(got_out)),
                   [w_1] + [shared(g) for g in got_up], [w_2] + [shared(g) for g in got_down])

        def my_tokens(values):
            return lax.dynamic_slice_in_dim(values, model_idx * batch, batch, 0).reshape(batch * seq, width)

        x_cur = my_tokens(x_in)
        saved_list = []
        for layer_idx in range(layer_count):
            x_cur, saved_acts = layer_forward(x_cur, step_emb[layer_idx], weights, batch, seq,
                                              layer_idx == layer_count - 1)
            saved_list.append(saved_acts)
        d_cur = my_tokens(cot_out)
        factors = {}
        pipe = GradientPipe(core_idx, chip_idx)

        def keep_factors(name, value, found):
            factors.setdefault(name, []).append(found)
            return value

        def send_gradient(name, value, found):
            keep_factors(name, value, found)
            p_layers, q_layers = zip(*factors[name])
            if name != 'down':
                value = pipe.stage(value)
            if name == 'qkv':
                for j, single in enumerate('qkv'):
                    pipe.begin(single, False, [[heads[j] for heads in p] for p in p_layers], q_layers)
            else:
                pipe.begin(name, name in ('down', 'out'), p_layers, q_layers)
            return pipe.after_sends(value)

        for layer_idx in reversed(range(layer_count)):
            d_cur = layer_backward(d_cur, step_emb[layer_idx], saved_list[layer_idx], weights, batch, seq,
                                   keep_factors if layer_idx else send_gradient)
        pipe.finish()
        grad_q, grad_k, grad_v, grad_wo, grad_up, grad_down = (
            pipe.result(name) for name in ('q', 'k', 'v', 'out', 'up', 'down'))
        d_mine = d_cur.reshape(batch, seq, width)
        d_x = ordered(model_idx, d_mine, swap_model(d_mine), 0)
        return grad_q, grad_k, grad_v, grad_wo, grad_up, grad_down, d_x

    return jax.shard_map(device_step, mesh=mesh,
                         in_specs=(spec_act, spec_act, spec_rep, spec_col, spec_col, spec_col, spec_row, spec_col, spec_row),
                         out_specs=(spec_col, spec_col, spec_col, spec_row, spec_col, spec_row, spec_act),
                         check_vma=False)
```

```python
import jax
import jax.numpy as jnp
from jax import lax
from jax.experimental import pallas as pl
from jax.experimental.layout import Layout, with_layout_constraint
from jax.experimental.pallas import tpu as pltpu
from jax.sharding import PartitionSpec as P


HEAD_DIM = 64
EPS_NORM = 1e-6
CHUNK = 1024
F32 = jnp.float32
BF16 = jnp.bfloat16


SWAP_MODEL = ((0, 1), (1, 0))
SWAP_CORE = ((0, 1), (1, 0), (2, 3), (3, 2))
SWAP_CHIP = ((0, 2), (2, 0), (1, 3), (3, 1))


def swap_model(values):
    return lax.ppermute(values, 'model', SWAP_MODEL)


def swap_core(values):
    return lax.ppermute(values, 'data', SWAP_CORE)


def swap_chip(values):
    return lax.ppermute(values, 'data', SWAP_CHIP)


def ordered(index, mine, other, axis):
    return jnp.where(index == 0, jnp.concatenate([mine, other], axis), jnp.concatenate([other, mine], axis))


def rms_norm(values):
    return values * lax.rsqrt(jnp.mean(values * values, axis=-1, keepdims=True) + EPS_NORM)


def dot(lhs, rhs, lhs_dim, rhs_dim):
    return lax.dot_general(lhs, rhs, (((lhs_dim,), (rhs_dim,)), ((), ())), preferred_element_type=F32)


PAIR = 2 * HEAD_DIM


def pair_masks(seq):
    lane = lax.broadcasted_iota(jnp.int32, (seq, PAIR), 1)
    first = jnp.where(lane < HEAD_DIM, 1.0, 0.0)
    return lane < HEAD_DIM, (first.astype(BF16), (1.0 - first).astype(BF16))


def stacked(values, masks):
    return jnp.concatenate([values * mask for mask in masks], axis=0)


def pair_probs(q_pair, k_stack):
    scores = dot(q_pair, k_stack, 1, 1) * (HEAD_DIM ** -0.5)
    half = scores.shape[1] // 2
    probs = []
    for part in (scores[:, :half], scores[:, half:]):
        weight = jnp.exp(part - jnp.max(part, axis=-1, keepdims=True))
        probs.append(weight / jnp.sum(weight, axis=-1, keepdims=True))
    return probs


def attn_forward_kernel(qkv_ref, out_ref):
    seq, width = out_ref.shape
    _, masks = pair_masks(seq)
    for start in range(0, width, PAIR):
        q_pair, k_pair, v_pair = (qkv_ref[:, i * width + start:i * width + start + PAIR] for i in range(3))
        probs = jnp.concatenate(pair_probs(q_pair, stacked(k_pair, masks)), axis=1).astype(BF16)
        out_ref[:, start:start + PAIR] = dot(probs, stacked(v_pair, masks), 1, 0).astype(BF16)


def attn_backward_kernel(qkv_ref, d_ref, out_ref):
    seq, width = d_ref.shape
    is_first, masks = pair_masks(seq)

    def merged(both):
        return jnp.where(is_first, both[:seq], both[seq:])

    for start in range(0, width, PAIR):
        q_pair, k_pair, v_pair = (qkv_ref[:, i * width + start:i * width + start + PAIR] for i in range(3))
        d_pair = d_ref[:, start:start + PAIR]
        k_stack = stacked(k_pair, masks)
        probs = pair_probs(q_pair, k_stack)
        d_probs = dot(d_pair, stacked(v_pair, masks), 1, 1).astype(BF16).astype(F32)
        d_scores = []
        for prob_f, d_prob in zip(probs, (d_probs[:, :seq], d_probs[:, seq:])):
            row_sum = jnp.sum(prob_f * d_prob, axis=-1, keepdims=True)
            d_scores.append(prob_f * (d_prob - row_sum) * (HEAD_DIM ** -0.5))
        d_scores = jnp.concatenate(d_scores, axis=1).astype(BF16)
        probs = jnp.concatenate(probs, axis=1).astype(BF16)
        grads = (dot(d_scores, k_stack, 1, 0), merged(dot(d_scores, q_pair, 0, 0)), merged(dot(probs, d_pair, 0, 0)))
        for i, grad in enumerate(grads):
            out_ref[:, i * width + start:i * width + start + PAIR] = grad.astype(BF16)


def per_sequence(kernel, seq, out_width, products, *operands):
    tokens = operands[0].shape[0]
    spec = lambda cols: pl.BlockSpec((seq, cols), lambda i: (i, 0))
    flops = products * 2 * tokens * seq * operands[-1].shape[1]
    moved = 2 * tokens * (out_width + sum(o.shape[1] for o in operands))
    return pl.pallas_call(
        kernel, grid=(tokens // seq,), in_specs=[spec(o.shape[1]) for o in operands], out_specs=spec(out_width),
        out_shape=jax.ShapeDtypeStruct((tokens, out_width), BF16),
        cost_estimate=pl.CostEstimate(flops=flops, bytes_accessed=moved, transcendentals=tokens * seq * 16),
        compiler_params=pltpu.CompilerParams(dimension_semantics=("arbitrary",)),
    )(*operands)


def attn_forward(qkv, seq):
    return per_sequence(attn_forward_kernel, seq, qkv.shape[1] // 3, 2, qkv)


def attn_backward(qkv, d_context, seq):
    return per_sequence(attn_backward_kernel, seq, qkv.shape[1], 12, qkv, d_context)


def layer_forward(x_cur, step_vec, weights, seq, last, take):
    w_qkv, w_out, w_up, w_down = weights
    x_f = x_cur.astype(F32) + step_vec.astype(F32)
    u_in = rms_norm(x_f).astype(BF16)
    qkv_own = dot(u_in, w_qkv[0], 1, 0).astype(BF16)
    qkv_own = take(qkv_own, 1)
    context_own = attn_forward(qkv_own, seq)
    context_own = take(context_own, 2)
    qkv_other = dot(u_in, w_qkv[1], 1, 0).astype(BF16)
    qkv_other = take(qkv_other, 1)
    context_other = attn_forward(qkv_other, seq)
    context_other = take(context_other, 1)
    qkv, context = [qkv_own, qkv_other], [context_own, context_other]
    attn_out = sum(dot(c, w, 1, 0) for c, w in zip(context, w_out))
    h_mid = (x_f + attn_out).astype(BF16)
    m_in = take(rms_norm(h_mid.astype(F32)).astype(BF16), 1)
    z_up = []
    for w in w_up:
        z_up.append(dot(m_in, w, 1, 0).astype(BF16))
    g_act = [jax.nn.gelu(z.astype(F32)).astype(BF16) for z in z_up]
    x_next = None
    if not last:
        x_next = (h_mid.astype(F32) + sum(dot(g, w, 1, 0) for g, w in zip(g_act, w_down))).astype(BF16)
    return x_next, (x_cur, u_in, qkv, context, h_mid, m_in, z_up, g_act)


def layer_backward(d_next, step_vec, saved_acts, weights, seq, step):
    w_qkv, w_out, w_up, w_down = weights
    x_cur, u_in, qkv, context, h_mid, m_in, z_up, g_act = saved_acts
    d_next = step('down', d_next, (g_act, d_next))
    d_up = []
    for z, w in zip(z_up, w_down):
        d_act = dot(d_next, w, 1, 1).astype(BF16)
        d_up.append(jax.vjp(jax.nn.gelu, z.astype(F32))[1](d_act.astype(F32))[0].astype(BF16))
        if len(d_up) == 2:
            d_up, d_next = step('', (d_up, d_next), None)
    d_up = step('up', d_up, (d_up, m_in))
    d_norm2 = sum(dot(d, w, 1, 1) for d, w in zip(d_up, w_up)).astype(BF16)
    norm_pull = jax.vjp(rms_norm, h_mid.astype(F32))[1]
    d_mid = (d_next.astype(F32) + norm_pull(d_norm2.astype(F32))[0]).astype(BF16)
    d_mid = step('out', d_mid, (context, d_mid))
    d_context = [dot(d_mid, w, 1, 1).astype(BF16) for w in w_out]
    d_qkv = [attn_backward(part, d, seq) for part, d in zip(qkv, d_context)]
    d_qkv = step('', d_qkv, None)
    d_qkv = step('qkv', d_qkv, (d_qkv, u_in))
    d_norm1 = sum(dot(d, w, 1, 1) for d, w in zip(d_qkv, w_qkv)).astype(BF16)
    x_f = x_cur.astype(F32) + step_vec.astype(F32)
    norm_pull_x = jax.vjp(rms_norm, x_f)[1]
    return (d_mid.astype(F32) + norm_pull_x(d_norm1.astype(F32))[0]).astype(BF16)


class GradientPipe:
    LAG = 2

    def __init__(self, core_idx, chip_idx, results):
        self.core_idx, self.chip_idx, self.results = core_idx, chip_idx, results
        self.blocks, self.sent, self.pending, self.count = [], [], [], 0

    def begin(self, names, p_first, p_layers, q_layers):
        q_all = jnp.concatenate(q_layers, axis=0)
        half_q = q_all.shape[1] // 2
        q_mine = lax.dynamic_slice_in_dim(q_all, self.core_idx * half_q, half_q, 1)
        q_mate = lax.dynamic_slice_in_dim(q_all, (1 - self.core_idx) * half_q, half_q, 1)

        def product(p_part, q_part):
            out = dot(p_part, q_part, 0, 0) if p_first else dot(q_part, p_part, 0, 0)
            return with_layout_constraint(out, Layout(major_to_minor=(0, 1)))

        own_p = list(zip(*(columns(parts[:1]) for parts in p_layers)))
        other_p = list(zip(*(columns(parts[1:]) for parts in p_layers)))
        for i, (own, other) in enumerate(zip(own_p, other_p)):
            number = len(self.blocks)
            if i:
                other, _ = lax.optimization_barrier((other, (self.sent[-2:-1], partial)))
            other = jnp.concatenate(other, axis=0)
            partial = product(other, q_mate)
            if self.sent:
                other, _ = lax.optimization_barrier((other, self.sent[-1]))
            send = swap_core(partial) + product(other, q_mine)
            self.sent.append(send)
            same = len(names) > 1
            block = dict(name=names[i] if same else names[0], at=0 if same else i * CHUNK, axis=1 if p_first else 0,
                         number=number, own=own, product=product, q_mine=q_mine, q_mate=q_mate)
            self.pending.append((number, 'model', block, swap_model(send)))
            self.blocks.append(block)
        for block in self.blocks[:self.LAG]:
            self.add_own(block, self.sent[-1])

    def add_own(self, block, after):
        if 'here' not in block:
            own, _ = lax.optimization_barrier((block['own'], after))
            own = jnp.concatenate(own, axis=0)
            block['here'] = swap_core(block['product'](own, block['q_mate'])) + block['product'](own, block['q_mine'])

    def after_sends(self, value):
        return lax.optimization_barrier((value, self.sent[-1]))[0]

    def write(self, block, part, core, chip):
        size = part.shape[block['axis']]
        start = core * (2 * size) + chip * size
        place = (block['at'], start) if block['axis'] else (start, block['at'])
        self.results[block['name']] = lax.dynamic_update_slice(self.results[block['name']], part, place)

    def stage(self, value=None):
        now, later = self.count, []
        self.count += 1
        ready = [item for item in self.pending if item[0] <= now]
        owns = [block['here'] for block in self.blocks[now:now + 1]]
        got, owns, value, self.results = lax.optimization_barrier(([item[3] for item in ready], owns, value, self.results))
        given = []
        here, there = self.chip_idx, 1 - self.chip_idx
        for (_, kind, block, _), arrived in zip(ready, got):
            axis = block['axis']
            if kind == 'model':
                total = owns[0] + arrived
                part = total.shape[axis] // 2
                block['mine'] = lax.dynamic_slice_in_dim(total, here * part, part, axis)
                give = lax.dynamic_slice_in_dim(total, there * part, part, axis)
                given.append(give)
                later.append((now + self.LAG, 'chip', block, swap_chip(give)))
            elif kind == 'chip':
                mine = block['mine'] + arrived
                given.append(mine)
                later.append((now + self.LAG, 'share', block, swap_chip(mine)))
                later.append((now + 1, 'core', dict(block, chip=here), swap_core(mine)))
                self.write(block, mine, self.core_idx, here)
            elif kind == 'share':
                later.append((now + 1, 'core', dict(block, chip=there), swap_core(arrived)))
                self.write(block, arrived, self.core_idx, there)
            else:
                self.write(block, arrived, 1 - self.core_idx, block['chip'])
        for block in self.blocks[:now + self.LAG + 1]:
            self.add_own(block, got)
        self.pending = [item for item in self.pending if item[0] > now] + later
        return lax.optimization_barrier((value, given))[0]

    def finish(self):
        while self.pending:
            self.stage()


def columns(parts):
    return [p[:, start:start + CHUNK] for p in parts for start in range(0, p.shape[1], CHUNK)]


def solution(mesh):
    spec_col = P(None, 'model')
    spec_row = P('model', None)
    spec_act = P('data', None, None)
    spec_rep = P(None, None)

    def device_step(x_in, cot_out, step_emb, w_q, w_k, w_v, w_o, w_1, w_2):
        model_idx = lax.axis_index('model')
        data_idx = lax.axis_index('data')
        chip_idx = data_idx // 2
        core_idx = data_idx % 2
        batch, seq, width = x_in.shape[0] // 2, x_in.shape[1], x_in.shape[2]
        layer_count = step_emb.shape[0]

        pieces = []

        def from_neighbour(shards, at, size):
            rows = size[0] // 4
            start = at[0] + (core_idx * 2 + chip_idx) * rows
            piece = jnp.concatenate([lax.dynamic_slice(s, (start, at[1]), (rows, size[1])) for s in shards], axis=1)
            if pieces:
                piece, _ = lax.optimization_barrier((piece, pieces[-1]))
            pieces.append(piece)
            return swap_model(piece)

        def shared(got):
            pair = ordered(chip_idx, got, swap_chip(got), 0)
            return ordered(core_idx, pair, swap_core(pair), 0)

        half = w_2.shape[0] // 2
        got_qkv = from_neighbour((w_q, w_k, w_v), (0, 0), w_q.shape)
        got_out = from_neighbour((w_o,), (0, 0), w_o.shape)
        got_up = [from_neighbour((w_1,), (0, at), (width, half)) for at in (0, half)]
        got_down = [from_neighbour((w_2,), (at, 0), (half, width)) for at in (0, half)]
        weights = [[jnp.concatenate([w_q, w_k, w_v], axis=1)], [w_o], [w_1], [w_2]]
        arriving = [got_qkv, got_out, *got_up, *got_down]
        into = [0, 1, 2, 2, 3, 3]
        results = {}
        for name, w in dict(q=w_q, k=w_k, v=w_v, out=w_o, up=w_1, down=w_2).items():
            results[name] = jnp.full(w.shape, float(len(results)), F32)

        def take(value, count):
            got, value = lax.optimization_barrier((arriving[:count], value))
            for piece, name in zip(got, into[:count]):
                weights[name].append(shared(piece))
            del arriving[:count], into[:count]
            return value

        def unchanged(value, count):
            return value

        def my_tokens(values):
            return lax.dynamic_slice_in_dim(values, model_idx * batch, batch, 0).reshape(batch * seq, width)

        x_cur = my_tokens(x_in)
        saved_list = []
        for layer_idx in range(layer_count):
            x_cur, saved_acts = layer_forward(x_cur, step_emb[layer_idx], weights, seq,
                                              layer_idx == layer_count - 1, unchanged if layer_idx else take)
            x_cur, results = lax.optimization_barrier((x_cur, results))
            saved_list.append(saved_acts)
        d_cur = my_tokens(cot_out)
        factors = {}
        pipe = GradientPipe(core_idx, chip_idx, results)

        def keep_factors(name, value, found):
            if name:
                factors.setdefault(name, []).append(found)
            return value

        def send_gradient(name, value, found):
            if not name:
                return pipe.stage(value)
            keep_factors(name, value, found)
            if name in ('up', 'out'):
                value = pipe.stage(value) if name == 'out' else value
            pipe.begin('qkv' if name == 'qkv' else (name,), name in ('down', 'out'), *zip(*factors[name]))
            value = pipe.after_sends(value)
            return pipe.stage(value) if name in ('up', 'qkv') else value

        for layer_idx in reversed(range(layer_count)):
            d_cur = layer_backward(d_cur, step_emb[layer_idx], saved_list[layer_idx], weights, seq,
                                   keep_factors if layer_idx else send_gradient)
        pipe.finish()
        grad_q, grad_k, grad_v, grad_wo, grad_up, grad_down = (
            pipe.results[name] for name in ('q', 'k', 'v', 'out', 'up', 'down'))
        d_mine = d_cur.reshape(batch, seq, width)
        d_x = ordered(model_idx, d_mine, swap_model(d_mine), 0)
        return grad_q, grad_k, grad_v, grad_wo, grad_up, grad_down, d_x

    return jax.shard_map(device_step, mesh=mesh,
                         in_specs=(spec_act, spec_act, spec_rep, spec_col, spec_col, spec_col, spec_row, spec_col, spec_row),
                         out_specs=(spec_col, spec_col, spec_col, spec_row, spec_col, spec_row, spec_act),
                         check_vma=False)
```
